32 devices in a mesh: seq: 4 (over z), blk: 4 (over y, core), uly: 2 (over x).
Axes of the slice: x: 2, y: 2, z: 4, core: 2. Of those that a mesh axis runs over, the one named last changes fastest.
Arguments:
- queries: bfloat16 [8192, 5120], P(('seq', 'blk', 'uly')), parts along dimension 0, may hold values from -60 to 60, as said below
- keys: bfloat16 [8192, 1024], P(('seq', 'blk', 'uly')), parts along dimension 0, may hold values from -60 to 60, as said below
- values: bfloat16 [8192, 1024], P(('seq', 'blk', 'uly')), parts along dimension 0, may hold values from -6 to 6
- positions: int32 [3, 8192], P(None, ('seq', 'blk', 'uly')), parts along dimension 1, may hold values from 0 to 526
- doc_lengths: int32 [32], P('seq'), parts along dimension 0, may hold values from 1 to 1024, 2048 in all
Outputs:
- attended: bfloat16 [8192, 5120], P(('seq', 'blk', 'uly')), parts along dimension 0
The draws below stay inside these ranges and needn't reach their ends.
There are 4 independent parts, one for each index of `seq`. The reference program is written for one: setup_inputs(seed, part) draws one part's arguments, and reference() takes and returns one part's arrays. A program takes and returns all parts, laid end to end along the dimension named above; each array names one. Nothing has to cross between parts.
Inputs may be any that keep to these rules, and one draw needn't show every extreme that they name: queries; the query rows hold values of order one, a few rows may be much larger. keys; the key rows hold values of order one, a few rows may be much larger.
All inputs are finite; a program needn't handle non-finite values.
Results may differ from the reference program's by a relative error of at most 0.0055.
Values may be sent and summed in bfloat16 or wider, within the bound.
A program may use at most 384 MiB of HBM per device.

```python
import math
import jax
import jax.numpy as jnp
import numpy as np
from jax import lax

KEY_VALUE_HEADS = 8
HEAD_SIZE = 128
QUERY_PER_KEY = 5
HQ = 40
NDOC = 8
PACKED_TOKENS = 2048


def draw_queries(key, part):
    frequency_base = jnp.clip(jax.random.normal(jax.random.fold_in(key, 1), (PACKED_TOKENS, HQ * HEAD_SIZE), jnp.float32), -6.0, 6.0)
    return frequency_base.astype(jnp.bfloat16)


def draw_keys(key, part):
    frequency_base = jnp.clip(jax.random.normal(jax.random.fold_in(key, 2), (PACKED_TOKENS, KEY_VALUE_HEADS * HEAD_SIZE), jnp.float32), -6.0, 6.0)
    return frequency_base.astype(jnp.bfloat16)


def draw_positions(key, part):
    index = jnp.arange(PACKED_TOKENS, dtype=jnp.int32)
    jitter = jax.random.randint(key, (3, PACKED_TOKENS), 0, 16)
    return (index[None, :] // 4 + jitter).astype(jnp.int32)


def shard_levels(own_key, shape, pieces, least, high):
    def one(axis_at, blocks):
        steps = jax.random.uniform(jax.random.fold_in(jax.random.fold_in(own_key, 6), axis_at), (blocks,), jnp.float32, least / len(pieces), high / len(pieces))
        return jnp.repeat(jnp.exp(steps), shape[axis_at] // blocks).reshape((-1,) + (1,) * (len(shape) - axis_at - 1))

    level = one(*pieces[0])
    for cut in pieces[1:]:
        level = level * one(*cut)
    return level


def profile(count, total, limit, lean):
    loads = [(1 << 20) // math.isqrt(standing ** lean) + 1 for standing in range(2, count + 1)]
    surplus, holding = total - limit - (count - 1), [1] * (count - 1)
    while surplus > 0:
        candidates = [i for i in range(count - 1) if holding[i] < limit]
        mass, remaining = sum([loads[i] for i in candidates]), surplus
        for i in candidates:
            more = min(limit - holding[i], max(1, remaining * loads[i] // mass), surplus)
            holding[i] = holding[i] + more
            surplus = surplus - more
    return np.array([limit] + holding)


def ragged(key, count, total, most, slope):
    if count == 2:
        one = jax.random.randint(key, (), max(1, total - most), min(most, total - 1) + 1)
        return jnp.stack([one, total - one])
    sizes = jnp.asarray(profile(count, total, most, slope), jnp.int32)
    pairs = (count - 1) // 2
    donor, sink = sizes[1:1 + 2 * pairs:2], sizes[2:2 + 2 * pairs:2]
    margin = jnp.minimum(donor - 1, most - sink)
    passed = jax.random.randint(jax.random.fold_in(key, 1), (pairs,), 0, 1 << 20) % (margin + 1)
    sizes = sizes.at[1:1 + 2 * pairs:2].set(donor - passed).at[2:2 + 2 * pairs:2].set(sink + passed)
    return sizes[jax.random.permutation(jax.random.fold_in(key, 2), count)]


def normal_values(own_key, shape, width, bound, shards=(), held_as=jnp.bfloat16):
    factor_of = shard_levels(own_key, shape, shards, -0.22, 0.18) if shards else 1.0
    values = jax.random.normal(own_key, shape, jnp.float32) * width * factor_of
    return jnp.minimum(jnp.maximum(values, -bound), bound).astype(held_as)


def setup_inputs(seed: int = 0, part: int = 0) -> dict:
    key_list = jax.random.split(jax.random.key(seed), 6)
    own_keys = jax.random.split(jax.random.fold_in(key_list[5], part), 6)
    return {
        "queries": draw_queries(jax.random.fold_in(jax.random.fold_in(key_list[5], part), 71), part),
        "keys": draw_keys(jax.random.fold_in(jax.random.fold_in(key_list[5], part), 71), part),
        "values": normal_values(own_keys[2], (PACKED_TOKENS, KEY_VALUE_HEADS * HEAD_SIZE), 1.0, 6.0, ((0, 8),)),
        "positions": draw_positions(jax.random.fold_in(jax.random.fold_in(key_list[5], part), 71), part),
        "doc_lengths": ragged(own_keys[4], NDOC, PACKED_TOKENS, PACKED_TOKENS // 2, 2).astype(jnp.int32),
    }


def apply_rotary(x, pos, heads):
    rows = x.shape[0]
    half = HEAD_SIZE // 2
    pair = jnp.arange(half, dtype=jnp.int32)
    freq = jnp.power(jnp.float32(1000000.0), -2.0 * pair.astype(jnp.float32) / HEAD_SIZE)
    place = pos.astype(jnp.float32)
    first = HEAD_SIZE // 8
    second = first + 3 * HEAD_SIZE // 16
    chosen = jnp.where(pair[None, :] < first, place[0][:, None], jnp.where(pair[None, :] < second, place[1][:, None], place[2][:, None]))
    angle = chosen * freq[None, :]
    cosine = jnp.cos(angle)[:, None, :]
    sine = jnp.sin(angle)[:, None, :]
    parts = x.reshape(rows, heads, HEAD_SIZE).astype(jnp.float32)
    lower = parts[..., :half]
    upper = parts[..., half:]
    turned = jnp.concatenate([lower * cosine - upper * sine, upper * cosine + lower * sine], axis=-1)
    return turned.reshape(rows, heads * HEAD_SIZE).astype(jnp.bfloat16)

def doc_starts(index, doc_lengths):
    ends = jnp.cumsum(doc_lengths).astype(jnp.int32)
    return lax.optimization_barrier(jnp.sum(jnp.where(ends[None, :] <= index[:, None], doc_lengths[None, :], 0), axis=1)).astype(jnp.int32)

def reference(queries, keys, values, positions, doc_lengths):
    query_rotated = apply_rotary(queries, positions, HQ)
    key_rotated = apply_rotary(keys, positions, KEY_VALUE_HEADS)
    index = jnp.arange(PACKED_TOKENS, dtype=jnp.int32)
    starts = doc_starts(index, doc_lengths)
    allowed = (index[None, :] <= index[:, None]) & (index[None, :] >= starts[:, None])
    scale = 1.0 / math.sqrt(HEAD_SIZE)
    grouped_query = jnp.transpose(query_rotated.reshape(PACKED_TOKENS, KEY_VALUE_HEADS, QUERY_PER_KEY, HEAD_SIZE), (1, 0, 2, 3))
    key_heads_view = jnp.transpose(key_rotated.reshape(PACKED_TOKENS, KEY_VALUE_HEADS, HEAD_SIZE), (1, 0, 2))
    value_heads_view = jnp.transpose(values.reshape(PACKED_TOKENS, KEY_VALUE_HEADS, HEAD_SIZE), (1, 0, 2))

    def one_head(operands):
        q_head, k_head, v_head = operands
        scores = jnp.einsum('rgd,bd->grb', q_head.astype(jnp.float32), k_head.astype(jnp.float32)) * scale
        scores = jnp.where(allowed[None], scores, -1e+30)
        best = lax.optimization_barrier(jnp.max(scores, axis=-1, keepdims=True))
        weights = jnp.where(allowed[None], jnp.exp(scores - best), 0.0)
        total = lax.optimization_barrier(jnp.sum(weights, axis=-1))
        weight_b = weights.astype(jnp.bfloat16)
        summed = jnp.einsum('grb,bd->grd', weight_b.astype(jnp.float32), v_head.astype(jnp.float32))
        return summed / total[..., None]
    result = lax.map(one_head, (grouped_query, key_heads_view, value_heads_view))
    return jnp.transpose(result, (2, 0, 1, 3)).reshape(PACKED_TOKENS, HQ * HEAD_SIZE).astype(jnp.bfloat16)
```

```python
import functools
import math

import jax
import jax.numpy as jnp
from jax import lax
from jax.experimental import pallas as pl
from jax.experimental.pallas import tpu as pltpu
from jax.sharding import PartitionSpec as P

HEAD_SIZE = 128
QUERY_PER_KEY = 5
AHEAD = 3


def rotary_tables(pos):
    half = HEAD_SIZE // 2
    pair = jnp.arange(half, dtype=jnp.int32)
    freq = jnp.power(jnp.float32(1000000.0), -2.0 * pair.astype(jnp.float32) / HEAD_SIZE)
    place = pos.astype(jnp.float32)
    first = HEAD_SIZE // 8
    second = first + 3 * HEAD_SIZE // 16
    chosen = jnp.where(
        pair[None, :] < first,
        place[0][:, None],
        jnp.where(pair[None, :] < second, place[1][:, None], place[2][:, None]),
    )
    angle = chosen * freq[None, :]
    cosine = jnp.cos(angle)
    sine = jnp.sin(angle)
    return jnp.concatenate([cosine, cosine], axis=1), jnp.concatenate([-sine, sine], axis=1)


def routes(blocks, lanes):
    count = blocks * lanes
    window = count // 2

    def place(r):
        return (r // lanes // 2, r % lanes), r // lanes % 2

    def member(chip, core):
        return (chip[0] * 2 + core) * lanes + chip[1]

    found = {}
    for s in range(count):
        home, own_core = place(s)
        wanting = set(range(s + 1, min(count, s + window + 1)))

        def entry(chip):
            if chip == home:
                return s
            for core in (own_core, 1 - own_core):
                if member(chip, core) in wanting:
                    return member(chip, core)
            return None

        for half in (0, 1):
            for r in sorted(wanting):
                chip, _ = place(r)
                source = entry(chip)
                if source == r:
                    options = []
                    if chip[1] != home[1]:
                        options.append(entry((chip[0], home[1])))
                    if chip[0] > home[0]:
                        options.append(entry((chip[0] - 1, chip[1])))
                    if half:
                        options.reverse()
                    options = [o for o in options if o is not None] + [s]
                    source = options[0]
                found.setdefault((source - s, r - source), (set(), set()))[half].add(source)
    return sorted(found.items(), key=lambda item: (-item[0][0], item[0][1]))


def among(me, devices):
    hit = jnp.bool_(False)
    for device in sorted(devices):
        hit = hit | (me == device)
    return hit


def kernel(
    plan, lanes, count, window, kheads,
    lengths, cosine, sine, keys, values, queries, out,
    kv, qbuf, obuf, bias, q_sem, o_sem, send_sem, recv_sem,
):
    rows = keys.shape[0]
    size = HEAD_SIZE
    group = QUERY_PER_KEY * size
    me = lax.axis_index("blk") * lanes + lax.axis_index("uly")
    fetch = pltpu.make_async_copy(queries, qbuf, q_sem)
    fetch.start()

    def where_is(r):
        return {"blk": lax.div(r, lanes), "uly": lax.rem(r, lanes)}

    def column(h, width):
        return pl.ds(pl.multiple_of(h * width, width), width)

    def fill_ones(i, carry):
        kv[lax.div(i, kheads), lax.rem(i, kheads), :, 2 * size:] = jnp.ones((rows, size), kv.dtype)
        return carry

    lax.fori_loop(0, (window + 1) * kheads, fill_ones, 0)
    for slot in range(1, window + 1):
        @pl.when(me < slot)
        def _():
            def clear(h, carry):
                kv[slot, h, :, : 2 * size] = jnp.zeros((rows, 2 * size), kv.dtype)
                return carry

            lax.fori_loop(0, kheads, clear, 0)

    barrier = pltpu.get_barrier_semaphore()
    for offset in range(1, count):
        peer = lax.rem(me + offset, count)
        pl.semaphore_signal(
            barrier, inc=1, device_id=where_is(peer), device_id_type=pl.DeviceIdType.MESH
        )

    def turn(x):
        x = x.astype(jnp.float32)
        return (x * cosine[...] + pltpu.roll(x, size // 2, 1) * sine[...]).astype(jnp.bfloat16)

    def own_block(h, carry):
        kv[0, h, :, :size] = turn(keys[:, column(h, size)])
        kv[0, h, :, size : 2 * size] = values[:, column(h, size)]
        return carry

    lax.fori_loop(0, kheads, own_block, 0)
    pl.semaphore_wait(barrier, count - 1)

    def copy_of(index, slot, step, h):
        return pltpu.make_async_remote_copy(
            src_ref=kv.at[slot, h, :, pl.ds(0, 2 * size)],
            dst_ref=kv.at[slot + step, h, :, pl.ds(0, 2 * size)],
            send_sem=send_sem.at[index, h],
            recv_sem=recv_sem.at[slot + step, h],
            device_id=where_is(me + step),
            device_id_type=pl.DeviceIdType.MESH,
        )

    def arrival(slot, h):
        return pltpu.make_async_remote_copy(
            src_ref=kv.at[slot, h, :, pl.ds(0, 2 * size)],
            dst_ref=kv.at[slot, h, :, pl.ds(0, 2 * size)],
            send_sem=send_sem.at[0, h],
            recv_sem=recv_sem.at[slot, h],
            device_id=where_is(me),
            device_id_type=pl.DeviceIdType.MESH,
        )

    def sends(senders, h):
        even, odd = senders
        if even == odd:
            return among(me, even)
        is_even = lax.rem(h, 2) == 0
        return (is_even & among(me, even)) | (jnp.logical_not(is_even) & among(me, odd))

    def send(slot, h):
        for index, ((from_slot, step), senders) in enumerate(plan):
            if from_slot == slot:
                @pl.when(sends(senders, h))
                def _():
                    copy_of(index, slot, step, h).start()

    def relays(slot, h):
        hit = jnp.bool_(False)
        for (from_slot, _), senders in plan:
            if from_slot == slot:
                hit = hit | sends(senders, h)
        return hit

    def first_sends(h, carry):
        send(0, h)
        return carry

    lax.fori_loop(0, AHEAD, first_sends, 0)

    row = lax.broadcasted_iota(jnp.int32, (rows, rows), 0) + me * rows
    col = lax.broadcasted_iota(jnp.int32, (rows, rows), 1)
    start = jnp.zeros((rows, rows), jnp.int32)
    end = jnp.int32(0)
    for d in range(lengths.shape[0]):
        end = end + lengths[d]
        start = start + jnp.where(row >= end, lengths[d], 0)
    for slot in range(window + 1):
        key = col + (me - slot) * rows
        allowed = (key >= start) & (key <= row)
        bias[:, slot * rows : (slot + 1) * rows] = jnp.where(allowed, 0.0, -1e30)

    fetch.wait()
    scale = math.log2(math.e) / math.sqrt(size)

    def head(h, carry):
        @pl.when(h + AHEAD < kheads)
        def _():
            send(0, h + AHEAD)

        for slot in range(window, 0, -1):
            @pl.when(relays(slot, h))
            def _():
                arrival(slot, h).wait_recv()
                send(slot, h)

        for slot in range(1, window + 1):
            @pl.when((me >= slot) & jnp.logical_not(relays(slot, h)))
            def _():
                arrival(slot, h).wait_recv()

        k_all = kv[:, h, :, :size].reshape((window + 1) * rows, size)
        v_all = kv[:, h, :, size:].reshape((window + 1) * rows, 2 * size)
        for g in range(QUERY_PER_KEY):
            at = pl.ds(pl.multiple_of(h * group + g * size, size), size)
            q = turn(qbuf[:, at])
            scores = lax.dot_general(
                q, k_all, (((1,), (1,)), ((), ())), preferred_element_type=jnp.float32
            )
            scores = scores + bias[...]
            best = jnp.max(scores, axis=1, keepdims=True)
            weights = jnp.exp2((scores - best) * scale).astype(jnp.bfloat16)
            summed = jnp.dot(weights, v_all, preferred_element_type=jnp.float32)
            obuf[:, at] = (summed[:, :size] / summed[:, size:]).astype(jnp.bfloat16)
        pltpu.make_async_copy(
            obuf.at[:, column(h, group)], out.at[:, column(h, group)], o_sem.at[h]
        ).start()
        return carry

    lax.fori_loop(0, kheads, head, 0)

    def finish(h, carry):
        for index, ((slot, step), senders) in enumerate(plan):
            @pl.when(sends(senders, h))
            def _():
                copy_of(index, slot, step, h).wait_send()

        pltpu.make_async_copy(
            obuf.at[:, column(h, group)], out.at[:, column(h, group)], o_sem.at[h]
        ).wait()
        return carry

    lax.fori_loop(0, kheads, finish, 0)


def local(blocks, lanes, queries, keys, values, positions, doc_lengths):
    rows = queries.shape[0]
    kheads = keys.shape[1] // HEAD_SIZE
    count = blocks * lanes
    window = count // 2
    plan = routes(blocks, lanes)
    cosine, sine = rotary_tables(positions)
    vmem = pl.BlockSpec(memory_space=pltpu.VMEM)
    anywhere = pl.BlockSpec(memory_space=pl.ANY)
    return pl.pallas_call(
        functools.partial(kernel, plan, lanes, count, window, kheads),
        out_shape=jax.ShapeDtypeStruct(queries.shape, jnp.bfloat16),
        in_specs=[pl.BlockSpec(memory_space=pltpu.SMEM), vmem, vmem, vmem, vmem, anywhere],
        out_specs=anywhere,
        scratch_shapes=[
            pltpu.VMEM((window + 1, kheads, rows, 3 * HEAD_SIZE), jnp.bfloat16),
            pltpu.VMEM(queries.shape, jnp.bfloat16),
            pltpu.VMEM(queries.shape, jnp.bfloat16),
            pltpu.VMEM((rows, (window + 1) * rows), jnp.float32),
            pltpu.SemaphoreType.DMA,
            pltpu.SemaphoreType.DMA((kheads,)),
            pltpu.SemaphoreType.DMA((len(plan), kheads)),
            pltpu.SemaphoreType.DMA((window + 1, kheads)),
        ],
        compiler_params=pltpu.CompilerParams(
            collective_id=0, has_side_effects=True, vmem_limit_bytes=60 * 1024 * 1024
        ),
        name="windowed_attention",
    )(doc_lengths, cosine, sine, keys, values, queries)


def solution(mesh):
    in_specs = (
        P(("seq", "blk", "uly"), None),
        P(("seq", "blk", "uly"), None),
        P(("seq", "blk", "uly"), None),
        P(None, ("seq", "blk", "uly")),
        P("seq"),
    )
    out_specs = P(("seq", "blk", "uly"), None)
    body = functools.partial(local, mesh.shape["blk"], mesh.shape["uly"])
    return jax.shard_map(body, mesh=mesh, in_specs=in_specs, out_specs=out_specs, check_vma=False)
```

```python
import functools
import math

import jax
import jax.numpy as jnp
import numpy as np
from jax import lax
from jax.experimental import pallas as pl
from jax.experimental.pallas import tpu as pltpu
from jax.sharding import PartitionSpec as P

HEAD_SIZE = 128
QUERY_PER_KEY = 5
AHEAD = 3
RELAY_AHEAD = 1


def frequencies():
    pair = np.arange(HEAD_SIZE) % (HEAD_SIZE // 2)
    return np.power(1000000.0, -2.0 * pair / HEAD_SIZE).astype(np.float32)[None, :]


def rotary_tables(places, freq):
    rows = places.shape[1]
    half = HEAD_SIZE // 2
    row = lax.broadcasted_iota(jnp.int32, (rows, rows), 0)
    col = lax.broadcasted_iota(jnp.int32, (rows, rows), 1)
    column = [
        jnp.sum(
            jnp.where(row == col, places[p : p + 1, :].astype(jnp.float32), 0.0),
            axis=1,
            keepdims=True,
        )
        for p in range(3)
    ]
    lane = lax.broadcasted_iota(jnp.int32, (rows, HEAD_SIZE), 1)
    upper = lane >= half
    pair = jnp.where(upper, lane - half, lane)
    first = HEAD_SIZE // 8
    second = first + 3 * HEAD_SIZE // 16
    chosen = jnp.where(pair < first, column[0], jnp.where(pair < second, column[1], column[2]))
    angle = chosen * freq
    turns = jnp.floor(angle * (2.0 / math.pi) + 0.5)
    rest = angle - turns * 1.5703125
    rest = rest - turns * 4.8351287841796875e-4
    rest = rest - turns * 3.138552419841289520264e-7
    rest = rest - turns * 6.07710050630396597660e-11
    quarter = turns.astype(jnp.int32) & 3
    square = rest * rest
    sine = rest + rest * square * (
        -1.0 / 6 + square * (1.0 / 120 + square * (-1.0 / 5040 + square * (1.0 / 362880)))
    )
    cosine = 1.0 + square * (
        -0.5 + square * (1.0 / 24 + square * (-1.0 / 720 + square * (1.0 / 40320)))
    )
    swap = (quarter & 1) == 1
    sin_turned = jnp.where(swap, cosine, sine)
    cos_turned = jnp.where(swap, sine, cosine)
    sin_turned = jnp.where(quarter >= 2, -sin_turned, sin_turned)
    cos_turned = jnp.where((quarter == 1) | (quarter == 2), -cos_turned, cos_turned)
    return cos_turned, jnp.where(upper, sin_turned, -sin_turned)


def routes(blocks, lanes):
    count = blocks * lanes
    window = count // 2

    def place(r):
        return (r // lanes // 2, r % lanes), r // lanes % 2

    def member(chip, core):
        return (chip[0] * 2 + core) * lanes + chip[1]

    found = {}
    for s in range(count):
        home, own_core = place(s)
        wanting = set(range(s + 1, min(count, s + window + 1)))

        def entry(chip):
            if chip == home:
                return s
            for core in (own_core, 1 - own_core):
                if member(chip, core) in wanting:
                    return member(chip, core)
            return None

        for half in (0, 1):
            for r in sorted(wanting):
                chip, _ = place(r)
                source = entry(chip)
                if source == r:
                    options = []
                    if chip[1] != home[1]:
                        options.append(entry((chip[0], home[1])))
                    if chip[0] > home[0]:
                        options.append(entry((chip[0] - 1, chip[1])))
                    if half:
                        options.reverse()
                    options = [o for o in options if o is not None] + [s]
                    source = options[0]
                found.setdefault((source - s, r - source), (set(), set()))[half].add(source)
    return sorted(found.items(), key=lambda item: (-item[0][0], item[0][1]))


def among(me, devices):
    hit = jnp.bool_(False)
    for device in sorted(devices):
        hit = hit | (me == device)
    return hit


def kernel(
    plan, lanes, count, window, kheads,
    lengths, places, freq, keys, values, queries, out,
    cosine, sine, kv, qbuf, bias, q_sem, send_sem, recv_sem,
):
    rows = keys.shape[0]
    size = HEAD_SIZE
    group = QUERY_PER_KEY * size
    me = lax.axis_index("blk") * lanes + lax.axis_index("uly")
    fetch = pltpu.make_async_copy(queries, qbuf, q_sem)
    fetch.start()

    def where_is(r):
        return {"blk": lax.div(r, lanes), "uly": lax.rem(r, lanes)}

    def column(h, width):
        return pl.ds(pl.multiple_of(h * width, width), width)

    def fill_ones(i, carry):
        kv[lax.div(i, kheads), lax.rem(i, kheads), :, 2 * size:] = jnp.ones((rows, size), kv.dtype)
        return carry

    lax.fori_loop(0, (window + 1) * kheads, fill_ones, 0)
    for slot in range(1, window + 1):
        @pl.when(me < slot)
        def _():
            def clear(h, carry):
                kv[slot, h, :, : 2 * size] = jnp.zeros((rows, 2 * size), kv.dtype)
                return carry

            lax.fori_loop(0, kheads, clear, 0)

    barrier = pltpu.get_barrier_semaphore()
    for offset in range(1, count):
        peer = lax.rem(me + offset, count)
        pl.semaphore_signal(
            barrier, inc=1, device_id=where_is(peer), device_id_type=pl.DeviceIdType.MESH
        )

    cosine[...], sine[...] = rotary_tables(places, freq[...])

    def turn(x):
        x = x.astype(jnp.float32)
        return (x * cosine[...] + pltpu.roll(x, size // 2, 1) * sine[...]).astype(jnp.bfloat16)

    def own_block(h, carry):
        kv[0, h, :, :size] = turn(keys[:, column(h, size)])
        kv[0, h, :, size : 2 * size] = values[:, column(h, size)]
        return carry

    lax.fori_loop(0, kheads, own_block, 0)
    pl.semaphore_wait(barrier, count - 1)

    def copy_of(index, slot, step, h):
        return pltpu.make_async_remote_copy(
            src_ref=kv.at[slot, h, :, pl.ds(0, 2 * size)],
            dst_ref=kv.at[slot + step, h, :, pl.ds(0, 2 * size)],
            send_sem=send_sem.at[index, h],
            recv_sem=recv_sem.at[slot + step, h],
            device_id=where_is(me + step),
            device_id_type=pl.DeviceIdType.MESH,
        )

    def arrival(slot, h):
        return pltpu.make_async_remote_copy(
            src_ref=kv.at[slot, h, :, pl.ds(0, 2 * size)],
            dst_ref=kv.at[slot, h, :, pl.ds(0, 2 * size)],
            send_sem=send_sem.at[0, h],
            recv_sem=recv_sem.at[slot, h],
            device_id=where_is(me),
            device_id_type=pl.DeviceIdType.MESH,
        )

    def sends(senders, h):
        even, odd = senders
        if even == odd:
            return among(me, even)
        is_even = lax.rem(h, 2) == 0
        return (is_even & among(me, even)) | (jnp.logical_not(is_even) & among(me, odd))

    def send(slot, h):
        for index, ((from_slot, step), senders) in enumerate(plan):
            if from_slot == slot:
                @pl.when(sends(senders, h))
                def _():
                    copy_of(index, slot, step, h).start()

    def relays(slot, h):
        hit = jnp.bool_(False)
        for (from_slot, _), senders in plan:
            if from_slot == slot:
                hit = hit | sends(senders, h)
        return hit

    def first_sends(h, carry):
        send(0, h)
        return carry

    lax.fori_loop(0, AHEAD, first_sends, 0)

    def forward(h, carry):
        for slot in range(window, 0, -1):
            @pl.when(relays(slot, h))
            def _():
                arrival(slot, h).wait_recv()
                send(slot, h)

        return carry

    row = lax.broadcasted_iota(jnp.int32, (rows, rows), 0) + me * rows
    col = lax.broadcasted_iota(jnp.int32, (rows, rows), 1)
    start = jnp.zeros((rows, rows), jnp.int32)
    end = jnp.int32(0)
    for d in range(lengths.shape[0]):
        end = end + lengths[d]
        start = start + jnp.where(row >= end, lengths[d], 0)
    for slot in range(window + 1):
        key = col + (me - slot) * rows
        allowed = (key >= start) & (key <= row)
        bias[:, slot * rows : (slot + 1) * rows] = jnp.where(allowed, 0.0, -1e30)

    fetch.wait()
    lax.fori_loop(0, RELAY_AHEAD, forward, 0)
    scale = math.log2(math.e) / math.sqrt(size)

    def head(h, carry):
        @pl.when(h + AHEAD < kheads)
        def _():
            send(0, h + AHEAD)

        @pl.when(h + RELAY_AHEAD < kheads)
        def _():
            forward(h + RELAY_AHEAD, carry)

        for slot in range(1, window + 1):
            @pl.when((me >= slot) & jnp.logical_not(relays(slot, h)))
            def _():
                arrival(slot, h).wait_recv()

        k_all = kv[:, h, :, :size].reshape((window + 1) * rows, size)
        v_all = kv[:, h, :, size:].reshape((window + 1) * rows, 2 * size)
        for g in range(QUERY_PER_KEY):
            at = pl.ds(pl.multiple_of(h * group + g * size, size), size)
            q = turn(qbuf[:, at])
            scores = lax.dot_general(
                q, k_all, (((1,), (1,)), ((), ())), preferred_element_type=jnp.float32
            )
            scores = scores + bias[...]
            best = jnp.max(scores, axis=1, keepdims=True)
            weights = jnp.exp2((scores - best) * scale).astype(jnp.bfloat16)
            summed = jnp.dot(weights, v_all, preferred_element_type=jnp.float32)
            out[:, at] = (summed[:, :size] / summed[:, size:]).astype(jnp.bfloat16)
        return carry

    lax.fori_loop(0, kheads, head, 0)

    def finish(h, carry):
        for index, ((slot, step), senders) in enumerate(plan):
            @pl.when(sends(senders, h))
            def _():
                copy_of(index, slot, step, h).wait_send()

        return carry

    lax.fori_loop(0, kheads, finish, 0)


def local(blocks, lanes, queries, keys, values, positions, doc_lengths):
    rows = queries.shape[0]
    kheads = keys.shape[1] // HEAD_SIZE
    count = blocks * lanes
    window = count // 2
    plan = routes(blocks, lanes)
    vmem = pl.BlockSpec(memory_space=pltpu.VMEM)
    anywhere = pl.BlockSpec(memory_space=pl.ANY)
    return pl.pallas_call(
        functools.partial(kernel, plan, lanes, count, window, kheads),
        out_shape=pltpu.VMEM(queries.shape, jnp.bfloat16),
        in_specs=[pl.BlockSpec(memory_space=pltpu.SMEM), vmem, vmem, vmem, vmem, anywhere],
        out_specs=vmem,
        scratch_shapes=[
            pltpu.VMEM((rows, HEAD_SIZE), jnp.float32),
            pltpu.VMEM((rows, HEAD_SIZE), jnp.float32),
            pltpu.VMEM((window + 1, kheads, rows, 3 * HEAD_SIZE), jnp.bfloat16),
            pltpu.VMEM(queries.shape, jnp.bfloat16),
            pltpu.VMEM((rows, (window + 1) * rows), jnp.float32),
            pltpu.SemaphoreType.DMA,
            pltpu.SemaphoreType.DMA((len(plan), kheads)),
            pltpu.SemaphoreType.DMA((window + 1, kheads)),
        ],
        compiler_params=pltpu.CompilerParams(
            collective_id=0, has_side_effects=True, vmem_limit_bytes=60 * 1024 * 1024
        ),
        name="windowed_attention",
    )(doc_lengths, positions, jnp.asarray(frequencies()), keys, values, queries)


def solution(mesh):
    in_specs = (
        P(("seq", "blk", "uly"), None),
        P(("seq", "blk", "uly"), None),
        P(("seq", "blk", "uly"), None),
        P(None, ("seq", "blk", "uly")),
        P("seq"),
    )
    out_specs = P(("seq", "blk", "uly"), None)
    body = functools.partial(local, mesh.shape["blk"], mesh.shape["uly"])
    return jax.shard_map(body, mesh=mesh, in_specs=in_specs, out_specs=out_specs, check_vma=False)
```
